32 devices in a mesh: beam: 2 (over x), fft: 16 (over z, y, core).
Axes of the slice: x: 2, y: 2, z: 4, core: 2. Of those that a mesh axis runs over, the one named last changes fastest.
Arguments:
- baseband: bfloat16 [4, 33554432], P('beam', 'fft'), parts along dimension 0, may hold values from -6 to 6
- spectrum_in: bfloat16 [4, 4096, 8192], P('beam', 'fft'), parts along dimension 0, may hold values from -6 to 6
- dm_index: int32 [1], replicated, may hold values from 0 to 63
Outputs:
- spectrum_out: bfloat16 [4, 4096, 8192], P('beam', 'fft'), parts along dimension 0
- smoothed: float32 [2, 2097152], P('beam', 'fft'), parts along dimension 0
The draws below stay inside these ranges and needn't reach their ends.
There are 2 independent parts, one for each index of `beam`. The reference program is written for one: setup_inputs(seed, part) draws one part's arguments, and reference() takes and returns one part's arrays. A program takes and returns all parts, laid end to end along the dimension named above; an argument that names none is the same for every part. Nothing has to cross between parts.
Inputs may be any that keep to these rules, and one draw needn't show every extreme that they name: `dm_index`: indices into the grid of 64 trial dispersion measures.
All inputs are finite; a program needn't handle non-finite values.
Results may differ from the reference program's by a relative error of at most 0.0019.
The reference program's roundings to bfloat16 on the way count: a program that leaves them out, or rounds other values in their place, can miss the bound.
Values may be sent and summed in bfloat16 or wider, within the bound.
A program may use at most 128 MiB of HBM per device.

```python
import math
import jax
import jax.numpy as jnp
from jax import lax

ROWS_OUTER = 32
ROWS_INNER = 128
COLS_OUTER = 64
COLS_INNER = 128
ROW_LENGTH = 4096
COLUMN_LENGTH = 8192
SEGMENT_SAMPLES = 33554432
TRIALS = 1
DM_GRID = 64
DECIMATE_FACTOR = 16
HALF_WIDTH = 16


def block_scale(own_key, dims, pieces, smallest, largest):
    factor_of = 1.0
    for dim, parts in pieces:
        heights = jax.random.uniform(jax.random.fold_in(jax.random.fold_in(own_key, 6), dim), (parts,), jnp.float32, smallest / len(pieces), largest / len(pieces))
        factor_of = factor_of * jnp.repeat(jnp.exp(heights), dims[dim] // parts).reshape((-1,) + (1,) * (len(dims) - 1 - dim))
    return factor_of


def gaussian(rng, shape, scale, reach, split=(), kind=jnp.bfloat16):
    array = scale * jax.random.normal(rng, shape, jnp.float32)
    if split:
        array = array * block_scale(rng, shape, split, -0.22, 0.18)
    return jnp.clip(array, -reach, reach).astype(kind)


def setup_inputs(seed: int = 0, part: int = 0) -> dict:
    streams_of = jax.random.split(jax.random.key(seed), 4)
    own_keys = jax.random.split(jax.random.fold_in(streams_of[3], part), 4)
    baseband = gaussian(own_keys[0], (2, SEGMENT_SAMPLES), 1.0, 6.0, ((1, 16),))
    spectrum_in = gaussian(own_keys[1], (2, ROW_LENGTH, COLUMN_LENGTH), 1.0, 6.0, ((1, 16),))
    dm_index = jax.random.randint(streams_of[2], (TRIALS,), 0, DM_GRID).astype(jnp.int32)
    return dict(baseband=baseband, spectrum_in=spectrum_in, dm_index=dm_index)


def dft_table(length, direction):
    positions = jnp.arange(length, dtype=jnp.int32)
    product = jnp.remainder(positions[:, None] * positions[None, :], length)
    radians = direction * 2.0 * math.pi / length * product.astype(jnp.float32)
    norm_scale = 1.0 / math.sqrt(length)
    cosine = jnp.cos(radians) * norm_scale
    sine_part = jnp.sin(radians) * norm_scale
    return jnp.stack([jnp.stack([cosine, sine_part]), jnp.stack([-sine_part, cosine])]).astype(jnp.bfloat16)

def radians_of(numer, modulus, direction):
    return direction * 2.0 * math.pi / modulus * jnp.remainder(numer, modulus).astype(jnp.float32)

def chirp_radians(freq_row, col_outer, col_inner, grid_steps):
    col_freq = col_outer + COLS_OUTER * col_inner
    whole_mod = 4.0 * DM_GRID * ROW_LENGTH * COLUMN_LENGTH
    cross_mod = 2 * DM_GRID * COLUMN_LENGTH
    square_mod = 4 * DM_GRID * COLUMN_LENGTH
    grid_float = grid_steps.astype(jnp.float32)
    row_square = (freq_row * freq_row).astype(jnp.float32)
    term_rows = grid_float[:, None, None, None] * row_square[None, :, None, None] / whole_mod
    cross = jnp.remainder(freq_row[:, None, None] * col_freq[None], cross_mod)
    cross = jnp.remainder(grid_steps[:, None, None, None] * cross[None], cross_mod)
    square = jnp.remainder(col_freq * col_freq, square_mod)
    square = jnp.remainder(grid_steps[:, None, None] * square[None], square_mod)
    high_part = square // 512
    low_part = square % 512
    square = jnp.remainder(jnp.remainder(ROW_LENGTH * high_part, square_mod) * 512 + ROW_LENGTH * low_part, square_mod)
    turns = term_rows + cross.astype(jnp.float32) / cross_mod + square[:, None].astype(jnp.float32) / square_mod
    return 2.0 * math.pi * turns

def rotate(values, radians):
    cosine = jnp.cos(radians)
    sine_part = jnp.sin(radians)
    real_part = values[:, 0] * cosine - values[:, 1] * sine_part
    imag_part = values[:, 0] * sine_part + values[:, 1] * cosine
    return jnp.stack([real_part, imag_part], axis=1).astype(jnp.bfloat16)

def dft_section(values, einsum_form, length, direction, radians):
    mixed_sum = jnp.einsum(einsum_form, values.astype(jnp.float32), dft_table(length, direction).astype(jnp.float32), precision=lax.Precision.HIGHEST)
    if radians is None:
        return mixed_sum.astype(jnp.bfloat16)
    return rotate(mixed_sum, radians)

def row_frequency(row_pos):
    return row_pos // ROWS_INNER + ROWS_OUTER * (row_pos % ROWS_INNER)

def forward_spectrum(baseband):
    values = baseband.reshape(1, 2, ROWS_OUTER, ROWS_INNER, COLUMN_LENGTH)
    outer_pos = jnp.arange(ROWS_OUTER, dtype=jnp.int32)[:, None]
    inner_pos = jnp.arange(ROWS_INNER, dtype=jnp.int32)[None, :]
    values = dft_section(values, 'dixyb,ioxk->dokyb', ROWS_OUTER, -1, radians_of(outer_pos * inner_pos, ROW_LENGTH, -1)[:, :, None])
    freq_row = outer_pos + ROWS_OUTER * inner_pos
    col_pos = jnp.arange(COLUMN_LENGTH, dtype=jnp.int32)
    values = dft_section(values, 'dikyb,ioyq->dokqb', ROWS_INNER, -1, radians_of(freq_row[:, :, None] * col_pos[None, None, :], SEGMENT_SAMPLES, -1))
    values = values.reshape(1, 2, ROW_LENGTH, COLS_OUTER, COLS_INNER)
    col_outer = jnp.arange(COLS_OUTER, dtype=jnp.int32)[:, None]
    col_inner = jnp.arange(COLS_INNER, dtype=jnp.int32)[None, :]
    values = dft_section(values, 'dimxy,ioxj->domjy', COLS_OUTER, -1, radians_of(col_outer * col_inner, COLUMN_LENGTH, -1))
    values = dft_section(values, 'dimjy,ioyq->domjq', COLS_INNER, -1, None)
    return values[0].reshape(2, ROW_LENGTH, COLUMN_LENGTH)

def dedisperse(spectrum, grid_steps):
    trial_total = grid_steps.shape[0]
    row_pos = jnp.arange(ROW_LENGTH, dtype=jnp.int32)
    freq_row = row_frequency(row_pos)
    col_outer = jnp.arange(COLS_OUTER, dtype=jnp.int32)[:, None]
    col_inner = jnp.arange(COLS_INNER, dtype=jnp.int32)[None, :]
    values = rotate(spectrum.astype(jnp.float32).reshape(1, 2, ROW_LENGTH, COLS_OUTER, COLS_INNER), chirp_radians(freq_row, col_outer, col_inner, grid_steps))
    values = dft_section(values, 'dimjq,ioqy->domjy', COLS_INNER, 1, radians_of(col_outer * col_inner, COLUMN_LENGTH, 1))
    col_time = COLS_INNER * col_outer + col_inner
    values = dft_section(values, 'dimjy,iojx->domxy', COLS_OUTER, 1, radians_of(freq_row[:, None, None] * col_time[None], SEGMENT_SAMPLES, 1))
    values = values.reshape(trial_total, 2, ROWS_OUTER, ROWS_INNER, COLUMN_LENGTH)
    outer_pos = jnp.arange(ROWS_OUTER, dtype=jnp.int32)[:, None]
    inner_pos = jnp.arange(ROWS_INNER, dtype=jnp.int32)[None, :]
    values = dft_section(values, 'dikqb,ioqy->dokyb', ROWS_INNER, 1, radians_of(outer_pos * inner_pos, ROW_LENGTH, 1)[:, :, None])
    values = dft_section(values, 'dikyb,iokx->doxyb', ROWS_OUTER, 1, None)
    wide = values.reshape(trial_total, 2, ROW_LENGTH, COLUMN_LENGTH).astype(jnp.float32)
    detected_power = wide[:, 0] * wide[:, 0] + wide[:, 1] * wide[:, 1]
    decimated_power = lax.optimization_barrier(jnp.mean(detected_power.reshape(trial_total, ROW_LENGTH, COLUMN_LENGTH // DECIMATE_FACTOR, DECIMATE_FACTOR), axis=3))
    return decimated_power.reshape(trial_total, SEGMENT_SAMPLES // DECIMATE_FACTOR)

def reference(baseband, spectrum_in, dm_index):
    spectrum_out = forward_spectrum(baseband)
    grid_steps = dm_index.astype(jnp.int32) + 1
    series_list = []
    for trial_pos in range(TRIALS):
        series_list.append(dedisperse(spectrum_in, grid_steps[trial_pos:trial_pos + 1]))
    series = jnp.concatenate(series_list, axis=0)
    padded = jnp.pad(series, ((0, 0), (HALF_WIDTH, HALF_WIDTH)))
    length = series.shape[1]
    window_sum = padded[:, 0:length]
    for offset in range(1, 2 * HALF_WIDTH + 1):
        window_sum = window_sum + padded[:, offset:offset + length]
    smoothed = window_sum / (2 * HALF_WIDTH + 1)
    return (spectrum_out, smoothed)
```

```python
import math

import jax
import jax.numpy as jnp
from jax import lax
from jax.experimental import pallas as pl
from jax.experimental.pallas import tpu as pltpu
from jax.sharding import PartitionSpec as P

ROWS_OUTER = 32
ROWS_INNER = 128
COLS_OUTER = 64
COLS_INNER = 128
ROW_LENGTH = 4096
COLUMN_LENGTH = 8192
SEGMENT_SAMPLES = 33554432
DM_GRID = 64
DECIMATE_FACTOR = 16
HALF_WIDTH = 16
BLOCK_ROWS = 16
GROUP = 16
F32 = jnp.float32
BF16 = jnp.bfloat16


def dft_table(length, direction):
    positions = jnp.arange(length, dtype=jnp.int32)
    product = jnp.remainder(positions[:, None] * positions[None, :], length)
    radians = direction * 2.0 * math.pi / length * product.astype(F32)
    norm_scale = 1.0 / math.sqrt(length)
    cosine = jnp.cos(radians) * norm_scale
    sine_part = jnp.sin(radians) * norm_scale
    return jnp.stack([jnp.stack([cosine, sine_part]), jnp.stack([-sine_part, cosine])]).astype(BF16)


def right_table(length, direction):
    return dft_table(length, direction).transpose(0, 2, 1, 3).reshape(2 * length, 2 * length)


def left_table(length, direction):
    return dft_table(length, direction).transpose(1, 3, 0, 2).reshape(2 * length, 2 * length)


def phases(numer, modulus, direction=1):
    radians = direction * 2.0 * math.pi / modulus * jnp.remainder(numer, modulus).astype(F32)
    return jnp.stack([jnp.cos(radians), jnp.sin(radians)])


def row_frequency(row_pos):
    return row_pos // ROWS_INNER + ROWS_OUTER * (row_pos % ROWS_INNER)


def times(a, b):
    return a[0] * b[0] - a[1] * b[1], a[0] * b[1] + a[1] * b[0]


def dot(a, b):
    return jnp.dot(a, b, preferred_element_type=F32)


def stacked(ref, place):
    return jnp.concatenate([ref[0, place, :].astype(BF16), ref[1, place, :].astype(BF16)], axis=0)


def keep(ref, place, pair):
    ref[0, place, :] = pair[0]
    ref[1, place, :] = pair[1]


def pieces(row_local):
    step = min(row_local, ROWS_INNER)
    return [
        (start, start // row_local, start % row_local, step)
        for start in range(0, ROW_LENGTH, step)
    ]


def front_kernel(spec, a_tab, q_tab, c_tab, cy_tab, x_tab, y_tab, e_in, e_out, out, first, second):
    rows = BLOCK_ROWS
    q = (q_tab[0], q_tab[1])
    for c in range(COLS_OUTER):
        cols = slice(c * COLS_INNER, (c + 1) * COLS_INNER)
        turn = times((a_tab[0, :, c : c + 1], a_tab[1, :, c : c + 1]), q)
        turn = times(turn, (c_tab[0, c : c + 1, :], c_tab[1, c : c + 1, :]))
        value = times((spec[0, :, cols].astype(F32), spec[1, :, cols].astype(F32)), turn)
        both = jnp.concatenate([value[0].astype(BF16), value[1].astype(BF16)], axis=1)
        mixed = dot(both, e_in[...])
        w1 = times(
            (mixed[:, :COLS_INNER], mixed[:, COLS_INNER:]),
            (cy_tab[0, c : c + 1, :], cy_tab[1, c : c + 1, :]),
        )
        keep(first, slice(c * rows, (c + 1) * rows), w1)
    for m in range(rows):
        mixed = dot(e_out[...], stacked(first, pl.ds(m, COLS_OUTER, stride=rows)))
        turn = times(
            (x_tab[0, 0, :, m : m + 1], x_tab[1, 0, :, m : m + 1]),
            (y_tab[0, m : m + 1, :], y_tab[1, m : m + 1, :]),
        )
        w2 = times((mixed[:COLS_OUTER], mixed[COLS_OUTER:]), turn)
        keep(second, slice(m * COLS_OUTER, (m + 1) * COLS_OUTER), w2)
    wide = out.shape[3] // COLS_INNER
    for x in range(COLS_OUTER):
        place = (x % wide) * COLS_INNER
        for part in range(2):
            out[x // wide, part, :, place : place + COLS_INNER] = second[
                part, pl.ds(x, rows, stride=COLS_OUTER), :
            ].astype(BF16)


def back_kernel(word, cy_tab, e_in, e_out, out, first, second):
    rows = BLOCK_ROWS
    wide = word.shape[3] // COLS_INNER
    for x in range(COLS_OUTER):
        place = (x % wide) * COLS_INNER
        for part in range(2):
            first[part, x * rows : (x + 1) * rows, :] = word[
                x // wide, part, :, place : place + COLS_INNER
            ].astype(F32)
    cy = (cy_tab[0], cy_tab[1])
    for m in range(rows):
        mixed = dot(e_in[...], stacked(first, pl.ds(m, COLS_OUTER, stride=rows)))
        v1 = times((mixed[:COLS_OUTER], mixed[COLS_OUTER:]), cy)
        both = jnp.concatenate([v1[0].astype(BF16), v1[1].astype(BF16)], axis=1)
        mixed = dot(both, e_out[...])
        keep(
            second,
            slice(m * COLS_OUTER, (m + 1) * COLS_OUTER),
            (mixed[:, :COLS_INNER], mixed[:, COLS_INNER:]),
        )
    for c in range(COLS_OUTER):
        cols = slice(c * COLS_INNER, (c + 1) * COLS_INNER)
        for part in range(2):
            out[part, :, cols] = second[part, pl.ds(c, rows, stride=COLS_OUTER), :].astype(BF16)


def rows_kernel(word, pn_tab, col_tab, py_tab, qy_tab, e_in, e_out, out, first, second):
    outer, inner = ROWS_OUTER, ROWS_INNER
    row_local = word.shape[2]
    for start, shard, local, step in pieces(row_local):
        for part in range(2):
            first[part, start : start + step, :] = word[
                shard, part, local : local + step, :
            ].astype(F32)
    for n in range(inner):
        mixed = dot(e_in[...], stacked(first, pl.ds(n, outer, stride=inner)))
        u1 = times(
            (mixed[:outer], mixed[outer:]), (pn_tab[0, :, n : n + 1], pn_tab[1, :, n : n + 1])
        )
        keep(second, slice(n * outer, (n + 1) * outer), u1)
    qy = (qy_tab[0], qy_tab[1])
    for p in range(outer):
        mixed = dot(e_out[...], stacked(second, pl.ds(p, inner, stride=outer)))
        turn = times(
            (col_tab[0, 0, :, p : p + 1], col_tab[1, 0, :, p : p + 1]),
            (py_tab[0, p : p + 1, :], py_tab[1, p : p + 1, :]),
        )
        u2 = times((mixed[:inner], mixed[inner:]), times(turn, qy))
        for start, shard, local, step in pieces(row_local):
            if start // inner == p:
                low = start % inner
                for part in range(2):
                    out[shard, part, local : local + step, :] = u2[part][low : low + step].astype(
                        BF16
                    )


def detect_kernel(word, np_tab, e_in, e_out, sum_tab, out, first):
    outer, inner = ROWS_OUTER, ROWS_INNER
    row_local = word.shape[2]
    for p in range(outer):
        held = [
            [
                word[shard, part, local : local + step, :]
                for start, shard, local, step in pieces(row_local)
                if start // inner == p
            ]
            for part in range(2)
        ]
        mixed = dot(e_in[...], jnp.concatenate(held[0] + held[1], axis=0))
        w3 = times(
            (mixed[:inner], mixed[inner:]), (np_tab[0, :, p : p + 1], np_tab[1, :, p : p + 1])
        )
        keep(first, slice(p * inner, (p + 1) * inner), w3)

    def gather(group, carry):
        total = jnp.zeros((outer, COLS_INNER), F32)
        for r in range(GROUP):
            mixed = dot(e_out[...], stacked(first, pl.ds(group * GROUP + r, outer, stride=inner)))
            signal = mixed.astype(BF16).astype(F32)
            power = signal[:outer] * signal[:outer] + signal[outer:] * signal[outer:]
            high = power.astype(BF16)
            low = (power - high.astype(F32)).astype(BF16)
            total = total + dot(high, sum_tab[r]) + dot(low, sum_tab[r])
        out[0, group] = total
        return carry

    lax.fori_loop(0, inner // GROUP, gather, 0)


def params():
    return pltpu.CompilerParams(
        dimension_semantics=("arbitrary",), vmem_limit_bytes=56 * 1024 * 1024
    )


def cost():
    return pl.CostEstimate(flops=12_000_000_000, bytes_accessed=40_000_000, transcendentals=0)


def whole_spec(array):
    zeros = (0,) * array.ndim
    return pl.BlockSpec(array.shape, lambda i: zeros)


def swap(values):
    return lax.all_to_all(values, "fft", split_axis=0, concat_axis=0, tiled=True)


def column_phases():
    c = jnp.arange(COLS_OUTER, dtype=jnp.int32)[:, None]
    y = jnp.arange(COLS_INNER, dtype=jnp.int32)[None, :]
    return c, y


def front(spectrum, grid_step, freq_row, shards):
    row_local = spectrum.shape[1]
    rows = BLOCK_ROWS
    blocks = row_local // rows
    c, y = column_phases()
    k = freq_row[:, None]
    cross_mod = 2 * DM_GRID * COLUMN_LENGTH
    square = (grid_step * (k * k)).astype(F32) / (4.0 * DM_GRID * ROW_LENGTH * COLUMN_LENGTH)
    cross = jnp.remainder(grid_step * (k * c.T), cross_mod).astype(F32) / cross_mod
    radians = 2.0 * math.pi * (square + cross)
    a_tab = jnp.stack([jnp.cos(radians), jnp.sin(radians)])
    q_tab = phases(grid_step * (k * y), cross_mod // COLS_OUTER)
    square_mod = 4 * DM_GRID * COLUMN_LENGTH // ROW_LENGTH
    column = c + COLS_OUTER * y
    c_tab = phases(grid_step * jnp.remainder(column * column, square_mod), square_mod)
    cy_tab = phases(c * y, COLUMN_LENGTH)
    x_tab = phases(freq_row.reshape(blocks, 1, rows) * c[None], SEGMENT_SAMPLES // COLS_INNER)
    y_tab = phases(k * y, SEGMENT_SAMPLES)
    e_in, e_out = right_table(COLS_INNER, 1), left_table(COLS_OUTER, 1)
    row_block = lambda width: pl.BlockSpec((2, rows, width), lambda i: (0, i, 0))
    return pl.pallas_call(
        front_kernel,
        grid=(blocks,),
        in_specs=[
            row_block(COLUMN_LENGTH),
            row_block(COLS_OUTER),
            row_block(COLS_INNER),
            whole_spec(c_tab),
            whole_spec(cy_tab),
            pl.BlockSpec((2, 1, COLS_OUTER, rows), lambda i: (0, i, 0, 0)),
            row_block(COLS_INNER),
            whole_spec(e_in),
            whole_spec(e_out),
        ],
        out_specs=pl.BlockSpec((shards, 2, rows, COLUMN_LENGTH // shards), lambda i: (0, 0, i, 0)),
        out_shape=jax.ShapeDtypeStruct((shards, 2, row_local, COLUMN_LENGTH // shards), BF16),
        scratch_shapes=[pltpu.VMEM((2, rows * COLS_OUTER, COLS_INNER), F32)] * 2,
        compiler_params=params(),
        cost_estimate=cost(),
        name="front",
    )(spectrum, a_tab, q_tab, c_tab, cy_tab, x_tab, y_tab, e_in, e_out)


def back(words):
    shards, _, row_local, width = words.shape
    rows = BLOCK_ROWS
    c, y = column_phases()
    cy_tab = phases(c * y, COLUMN_LENGTH, -1)
    e_in, e_out = left_table(COLS_OUTER, -1), right_table(COLS_INNER, -1)
    return pl.pallas_call(
        back_kernel,
        grid=(row_local // rows,),
        in_specs=[
            pl.BlockSpec((shards, 2, rows, width), lambda i: (0, 0, i, 0)),
            whole_spec(cy_tab),
            whole_spec(e_in),
            whole_spec(e_out),
        ],
        out_specs=pl.BlockSpec((2, rows, COLUMN_LENGTH), lambda i: (0, i, 0)),
        out_shape=jax.ShapeDtypeStruct((2, row_local, COLUMN_LENGTH), BF16),
        scratch_shapes=[pltpu.VMEM((2, rows * COLS_OUTER, COLS_INNER), F32)] * 2,
        compiler_params=params(),
        cost_estimate=cost(),
        name="back",
    )(words, cy_tab, e_in, e_out)


def row_section(words, device_index):
    shards, _, row_local, width = words.shape
    tiles = width // COLS_INNER
    p = jnp.arange(ROWS_OUTER, dtype=jnp.int32)
    q = jnp.arange(ROWS_INNER, dtype=jnp.int32)
    y = jnp.arange(COLS_INNER, dtype=jnp.int32)
    pn_tab = phases(p[:, None] * q[None, :], ROW_LENGTH, -1)
    tile = device_index * tiles + jnp.arange(tiles, dtype=jnp.int32)
    k = p[None, :] + ROWS_OUTER * q[:, None]
    col_tab = phases(tile[:, None, None] * k[None], SEGMENT_SAMPLES // COLS_INNER, -1)
    py_tab = phases(p[:, None] * y[None, :], SEGMENT_SAMPLES, -1)
    qy_tab = phases(q[:, None] * y[None, :], SEGMENT_SAMPLES // ROWS_OUTER, -1)
    e_in, e_out = left_table(ROWS_OUTER, -1), left_table(ROWS_INNER, -1)
    block = pl.BlockSpec((shards, 2, row_local, COLS_INNER), lambda i: (0, 0, 0, i))
    return pl.pallas_call(
        rows_kernel,
        grid=(tiles,),
        in_specs=[
            block,
            whole_spec(pn_tab),
            pl.BlockSpec((2, 1, ROWS_INNER, ROWS_OUTER), lambda i: (0, i, 0, 0)),
            whole_spec(py_tab),
            whole_spec(qy_tab),
            whole_spec(e_in),
            whole_spec(e_out),
        ],
        out_specs=block,
        out_shape=jax.ShapeDtypeStruct(words.shape, BF16),
        scratch_shapes=[pltpu.VMEM((2, ROW_LENGTH, COLS_INNER), F32)] * 2,
        compiler_params=params(),
        cost_estimate=cost(),
        name="row_section",
    )(words, pn_tab, col_tab, py_tab, qy_tab, e_in, e_out)


def detect(words):
    shards, _, row_local, width = words.shape
    tiles = width // COLS_INNER
    p = jnp.arange(ROWS_OUTER, dtype=jnp.int32)
    n = jnp.arange(ROWS_INNER, dtype=jnp.int32)
    np_tab = phases(n[:, None] * p[None, :], ROW_LENGTH)
    e_in, e_out = left_table(ROWS_INNER, 1), left_table(ROWS_OUTER, 1)
    lane = jnp.arange(COLS_INNER, dtype=jnp.int32)
    short = COLS_INNER // DECIMATE_FACTOR
    slot = jnp.arange(GROUP, dtype=jnp.int32)[:, None] * short + lane[None, :] // DECIMATE_FACTOR
    sum_tab = ((slot[:, :, None] == lane[None, None, :]) / DECIMATE_FACTOR).astype(BF16)
    groups = ROWS_INNER // GROUP
    power = pl.pallas_call(
        detect_kernel,
        grid=(tiles,),
        in_specs=[
            pl.BlockSpec((shards, 2, row_local, COLS_INNER), lambda i: (0, 0, 0, i)),
            whole_spec(np_tab),
            whole_spec(e_in),
            whole_spec(e_out),
            whole_spec(sum_tab),
        ],
        out_specs=pl.BlockSpec((1, groups, ROWS_OUTER, COLS_INNER), lambda i: (i, 0, 0, 0)),
        out_shape=jax.ShapeDtypeStruct((tiles, groups, ROWS_OUTER, COLS_INNER), F32),
        scratch_shapes=[pltpu.VMEM((2, ROW_LENGTH, COLS_INNER), F32)],
        compiler_params=params(),
        cost_estimate=cost(),
        name="detect",
    )(words, np_tab, e_in, e_out, sum_tab)
    power = power.astype(BF16).reshape(tiles, groups, ROWS_OUTER, GROUP, short)
    return power.transpose(2, 1, 3, 0, 4).reshape(ROW_LENGTH, tiles * short)


def smooth(series):
    count = lax.axis_size("fft")
    forward = [(i, i + 1) for i in range(count - 1)]
    backward = [(target, source) for source, target in forward]
    low = lax.ppermute(series[-HALF_WIDTH:], "fft", forward)
    high = lax.ppermute(series[:HALF_WIDTH], "fft", backward)
    length = series.shape[0]
    frames = series.reshape(length // 128, 128)
    before = jnp.concatenate([low[None], frames[:-1, -HALF_WIDTH:]], axis=0)
    after = jnp.concatenate([frames[1:, :HALF_WIDTH], high[None]], axis=0)
    frames = jnp.concatenate([before, frames, after], axis=1)
    source = jnp.arange(128 + 2 * HALF_WIDTH, dtype=jnp.int32)[:, None]
    target = jnp.arange(128, dtype=jnp.int32)[None, :]
    band = ((source >= target) & (source <= target + 2 * HALF_WIDTH)).astype(BF16)
    return (dot(frames, band) / (2 * HALF_WIDTH + 1)).reshape(length)


def on_device(baseband, spectrum_in, dm_index):
    device_index = lax.axis_index("fft")
    shards = lax.axis_size("fft")
    row_local = spectrum_in.shape[1]
    width = COLUMN_LENGTH // shards
    word = baseband.reshape(2, row_local, shards, width).transpose(2, 0, 1, 3)
    word, spectrum_in = lax.optimization_barrier((word, spectrum_in))
    time_rows = swap(word)
    grid_steps = dm_index + 1
    row_pos = device_index * row_local + jnp.arange(row_local, dtype=jnp.int32)
    freq_row = row_frequency(row_pos)
    trials = dm_index.shape[0]
    fronts = [front(spectrum_in, grid_steps[t], freq_row, shards) for t in range(trials)]
    time_rows, *fronts = lax.optimization_barrier((time_rows, *fronts))
    moved = [swap(item) for item in fronts]
    partial = row_section(time_rows, device_index)
    partial, *moved = lax.optimization_barrier((partial, *moved))
    partial = swap(partial)
    powers = [detect(item) for item in moved]
    partial, *powers = lax.optimization_barrier((partial, *powers))
    results = []
    for power in powers:
        power = swap(power.reshape(shards, row_local, width // DECIMATE_FACTOR))
        results.append(smooth(power.transpose(1, 0, 2).reshape(-1)))
    return back(partial), jnp.stack(results)


def solution(mesh):
    placed = (P("beam", "fft"), P("beam", "fft", None), P())
    return jax.shard_map(
        on_device,
        mesh=mesh,
        in_specs=placed,
        out_specs=(P("beam", "fft", None), P("beam", "fft")),
        check_vma=False,
    )
```
